32 devices in a mesh: groups: 1, role: 2 (over core), dev: 16 (over z, y, x).
Axes of the slice: x: 2, y: 2, z: 4, core: 2. Of those that a mesh axis runs over, the one named last changes fastest.
Arguments:
- prompt_hidden: bfloat16 [4096, 4096], P(('groups', 'dev')), may hold values from -6 to 6
- norm_gain: float32 [4096], replicated, may hold values from 0.25 to 1.75
- kv_weight: bfloat16 [4096, 4, 2, 128], P(None, 'role'), may hold values from -0.09375 to 0.09375
- prompt_excess: int32 [4], P('groups'), may hold values from 1 to 1536, 2048 in all
- prompt_owner: int32 [4], P('groups'), may hold values from 0 to 15, as said below
- response_counts: int32 [4], P('groups'), may hold values from 1 to 5, as said below
- queries: bfloat16 [256, 16, 128], P(('groups', 'dev'), 'role'), may hold values from -256 to 256
- new_kv: bfloat16 [256, 4, 2, 128], P(('groups', 'dev'), 'role'), may hold values from -6 to 6
- response_cache: bfloat16 [256, 256, 4, 2, 128], P(('groups', 'dev'), None, 'role'), may hold values from -6 to 6
- positions: int32 [256], P(('groups', 'dev')), may hold values from 0 to 256
- out_weight: bfloat16 [16, 128, 4096], P('role', None, 'dev'), may hold values from -0.125 to 0.125
Outputs:
- attended: bfloat16 [256, 16, 128], P(('groups', 'dev'), 'role')
- block_out: bfloat16 [256, 4096], P(('groups', 'role'), 'dev')
The draws below stay inside these ranges and needn't reach their ends.
Inputs may be any that keep to these rules, and one draw needn't show every extreme that they name: `prompt_owner`: no device along dev owns more than two prompts, and some device owns exactly two. `response_counts`: some prompt has exactly 5 responses.
All inputs are finite; a program needn't handle non-finite values.
Results may differ from the reference program's by a relative error of at most 0.0065.
Values may be sent and summed in bfloat16 or wider, within the bound.
A program may use at most 192 MiB of HBM per device.

```python
import math
import jax
import jax.numpy as jnp
import numpy as np
from jax import lax

D = 4096
HEAD = 128
KV_HEADS = 4
Q_HEADS = 16
RESP = 5
PROMPT_MIN = 512
SEQ_DEV = 16
CTX = 256
TOKENS = 4096
PROMPTS = 4
LONGEST = 2048
SEQS = 256
N_DEV = 16


def owners_counts(key):
    folded = jax.random.fold_in(key, 11)
    seat_key, order_key, count_key, place_key = jax.random.split(folded, 4)
    seating = jax.random.permutation(seat_key, 2 * N_DEV).astype(jnp.int32)
    partner = jnp.bitwise_xor(seating[0], 1)
    where_partner = jnp.argmax(seating == partner)
    seating = seating.at[where_partner].set(seating[1])
    seating = seating.at[1].set(partner)
    chosen = seating[:PROMPTS] // 2
    picked = chosen[2] if PROMPTS > 2 else chosen[0]
    last_device = N_DEV - 1
    chosen = jnp.where(chosen == picked, last_device, jnp.where(chosen == last_device, picked, chosen))
    shuffle = jax.random.permutation(order_key, PROMPTS)
    owners = chosen[shuffle].astype(jnp.int32)
    counts = jax.random.randint(count_key, (PROMPTS,), 1, RESP + 1)
    placed = jax.random.randint(place_key, (), 0, PROMPTS)
    counts = counts.at[placed].set(RESP)
    return (owners, counts.astype(jnp.int32))


def draw_prompt_owner(key, part):
    return owners_counts(key)[0]


def draw_response_counts(key, part):
    return owners_counts(key)[1]


def draw_queries(key, part):
    values = jax.random.normal(key, (SEQS, Q_HEADS, HEAD), jnp.float32)
    values = jnp.clip(values, -4.0, 4.0)
    return values.astype(jnp.bfloat16)


def with_ends(result, own_key, smallest, largest):
    dims = result.shape
    index_at = [jax.random.randint(jax.random.fold_in(own_key, axis), (), 0, dims[axis]) for axis in range(len(dims))]
    result = result.at[tuple(index_at)].set(smallest)
    longest = dims.index(max(dims))
    index_at[longest] = (index_at[longest] + 1) % dims[longest]
    return result.at[tuple(index_at)].set(largest)


def levels(own_key, dims, cuts, least, high):
    gain = 1.0
    for dim, shards_of in cuts:
        heights = jax.random.uniform(jax.random.fold_in(jax.random.fold_in(own_key, 6), dim), (shards_of,), jnp.float32, least / len(cuts), high / len(cuts))
        gain = gain * jnp.repeat(jnp.exp(heights), dims[dim] // shards_of).reshape((-1,) + (1,) * (len(dims) - 1 - dim))
    return gain


def length_profile(number_of, total, reach, slope):
    loads = [(1 << 20) // math.isqrt(rank ** slope) + 1 for rank in range(2, number_of + 1)]
    surplus, holding = total - reach - (number_of - 1), [1] * (number_of - 1)
    while surplus > 0:
        candidates = [i for i in range(number_of - 1) if holding[i] < reach]
        mass, budget = sum([loads[i] for i in candidates]), surplus
        for i in candidates:
            addition = min(reach - holding[i], max(1, budget * loads[i] // mass), surplus)
            holding[i] = holding[i] + addition
            surplus = surplus - addition
    return np.array([reach] + holding)


def ragged(key, number_of, total, reach, skew):
    if number_of == 2:
        one = jax.random.randint(key, (), max(1, total - reach), min(reach, total - 1) + 1)
        return jnp.stack([one, total - one])
    sizes = jnp.asarray(length_profile(number_of, total, reach, skew), jnp.int32)
    pairs = (number_of - 1) // 2
    source_of, sink = sizes[1:1 + 2 * pairs:2], sizes[2:2 + 2 * pairs:2]
    margin = jnp.minimum(source_of - 1, reach - sink)
    passed = jax.random.randint(jax.random.fold_in(key, 1), (pairs,), 0, 1 << 20) % (margin + 1)
    sizes = sizes.at[1:1 + 2 * pairs:2].set(source_of - passed).at[2:2 + 2 * pairs:2].set(sink + passed)
    return sizes[jax.random.permutation(jax.random.fold_in(key, 2), number_of)]


def normal_values(key, dims, spread, most, cuts=(), kind=jnp.bfloat16):
    gain = levels(key, dims, cuts, -0.22, 0.18) if cuts else 1.0
    values = jax.random.normal(key, dims, jnp.float32) * spread * gain
    return jnp.minimum(jnp.maximum(values, -most), most).astype(kind)


def setup_inputs(seed: int = 0, part: int = 0) -> dict:
    key_of = jax.random.split(jax.random.key(seed), 12)
    own_keys = jax.random.split(jax.random.fold_in(key_of[11], part), 12)
    return {
        "prompt_hidden": normal_values(own_keys[0], (TOKENS, D), 1.0, 6.0, ((0, 16),)),
        "norm_gain": jnp.clip(1.0 + 0.15 * jax.random.normal(key_of[1], (D,), jnp.float32), 0.25, 1.75),
        "kv_weight": normal_values(key_of[2], (D, KV_HEADS, 2, HEAD), D ** -0.5, 0.09375, ((1, 2),)),
        "prompt_excess": ragged(own_keys[3], PROMPTS, TOKENS - PROMPTS * PROMPT_MIN, LONGEST - PROMPT_MIN, 2).astype(jnp.int32),
        "prompt_owner": draw_prompt_owner(jax.random.fold_in(jax.random.fold_in(key_of[11], part), 71), part),
        "response_counts": draw_response_counts(jax.random.fold_in(jax.random.fold_in(key_of[11], part), 71), part),
        "queries": draw_queries(jax.random.fold_in(jax.random.fold_in(key_of[11], part), 71), part),
        "new_kv": normal_values(own_keys[7], (SEQS, KV_HEADS, 2, HEAD), 1.0, 6.0, ((0, 16), (1, 2))),
        "response_cache": normal_values(own_keys[8], (SEQS, CTX, KV_HEADS, 2, HEAD), 1.0, 6.0, ((0, 16), (2, 2))),
        "positions": with_ends(jax.random.randint(own_keys[9], (SEQS,), 0, CTX + 1), jax.random.fold_in(own_keys[9], 1), 0, CTX).astype(jnp.int32),
        "out_weight": normal_values(key_of[10], (Q_HEADS, HEAD, D), (Q_HEADS * HEAD) ** -0.5, 0.125, ((0, 2), (2, 16))),
    }


rope_base = 500000.0

def rotate(vectors, offsets):
    half = vectors.shape[-1] // 2
    freq = rope_base ** (-jnp.arange(half, dtype=jnp.float32) * 2.0 / vectors.shape[-1])
    angles = offsets.astype(jnp.float32)[:, None] * freq[None, :]
    cosine = jnp.cos(angles)[:, None, :]
    sine = jnp.sin(angles)[:, None, :]
    first = vectors[..., :half]
    second = vectors[..., half:]
    return jnp.concatenate([first * cosine - second * sine, second * cosine + first * sine], axis=-1)

def prompt_layout(prompt_excess, token_index):
    lengths = PROMPT_MIN + prompt_excess
    ends = jnp.cumsum(lengths).astype(jnp.int32)
    starts = (ends - lengths).astype(jnp.int32)
    prompt_id = lax.optimization_barrier(jnp.sum((token_index[:, None] >= ends[None, :]).astype(jnp.int32), axis=1))
    member = prompt_id[:, None] == jnp.arange(lengths.shape[0], dtype=jnp.int32)[None, :]
    offsets = token_index - lax.optimization_barrier(jnp.sum(jnp.where(member, starts[None, :], 0), axis=1))
    return (member, offsets, starts, lengths)

def slot_prompts(owner, counts, slot_device, slot_index):
    order = jnp.arange(owner.shape[0], dtype=jnp.int32)
    earlier = (owner[:, None] == owner[None, :]) & (order[None, :] < order[:, None])
    first = lax.optimization_barrier(jnp.sum(jnp.where(earlier, counts[None, :], 0), axis=1))
    match = (owner[None, :] == slot_device[:, None]) & (first[None, :] <= slot_index[:, None]) & (slot_index[:, None] < first[None, :] + counts[None, :])
    present = jnp.any(match, axis=1)
    chosen = lax.optimization_barrier(jnp.sum(jnp.where(match, order[None, :], 0), axis=1)).astype(jnp.int32)
    return (chosen, present)

def reference(prompt_hidden, norm_gain, kv_weight, prompt_excess, prompt_owner, response_counts, queries, new_kv, response_cache, positions, out_weight):
    token_index = jnp.arange(TOKENS, dtype=jnp.int32)
    member, offsets, starts, lengths = prompt_layout(prompt_excess, token_index)
    hidden = prompt_hidden.astype(jnp.float32)
    normed = (hidden * lax.rsqrt(lax.optimization_barrier(jnp.mean(hidden * hidden, axis=-1, keepdims=True)) + 1e-05) * norm_gain).astype(jnp.bfloat16)
    projected = jnp.dot(normed, kv_weight.reshape(D, KV_HEADS * 2 * HEAD), preferred_element_type=jnp.float32)
    projected = projected.reshape(TOKENS, KV_HEADS, 2, HEAD)
    prompt_keys = rotate(projected[:, :, 0], offsets).astype(jnp.bfloat16)
    prompt_values = projected[:, :, 1].astype(jnp.bfloat16)
    slot_all = jnp.arange(SEQS, dtype=jnp.int32)
    chosen, present = slot_prompts(prompt_owner, response_counts, slot_all // SEQ_DEV, slot_all % SEQ_DEV)
    group = Q_HEADS // KV_HEADS

    def one_slot(inputs):
        query, fresh, cache, position, pick, live = inputs
        begin = jnp.minimum(starts[pick], TOKENS - LONGEST).astype(jnp.int32)
        window_keys = lax.dynamic_slice_in_dim(prompt_keys, begin, LONGEST, 0)
        window_values = lax.dynamic_slice_in_dim(prompt_values, begin, LONGEST, 0)
        token_ids = begin + jnp.arange(LONGEST, dtype=jnp.int32)
        prompt_valid = live & (token_ids >= starts[pick]) & (token_ids < starts[pick] + lengths[pick])
        cache_valid = jnp.arange(CTX, dtype=jnp.int32) < position
        all_keys = jnp.concatenate([window_keys, cache[:, :, 0], fresh[None, :, 0]], axis=0)
        all_values = jnp.concatenate([window_values, cache[:, :, 1], fresh[None, :, 1]], axis=0)
        valid = jnp.concatenate([prompt_valid, cache_valid, jnp.ones((1,), dtype=bool)], axis=0)
        grouped = query.astype(jnp.float32).reshape(KV_HEADS, group, HEAD)
        scores = jnp.einsum('ngd,lnd->ngl', grouped, all_keys.astype(jnp.float32)) * HEAD ** (-0.5)
        scores = jnp.where(valid[None, None, :], scores, -1e+30)
        peak = lax.optimization_barrier(jnp.max(scores, axis=-1, keepdims=True))
        weights = jnp.where(valid[None, None, :], jnp.exp(scores - peak), 0.0)
        total = lax.optimization_barrier(jnp.sum(weights, axis=-1))
        rounded = lax.optimization_barrier(weights.astype(jnp.bfloat16)).astype(jnp.float32)
        mixed = jnp.einsum('ngl,lnd->ngd', rounded, all_values.astype(jnp.float32))
        return (mixed / total[..., None]).reshape(Q_HEADS, HEAD).astype(jnp.bfloat16)
    attended = lax.map(one_slot, (queries, new_kv, response_cache, positions, chosen, present))
    block_out = jnp.dot(attended.reshape(SEQS, Q_HEADS * HEAD), out_weight.reshape(Q_HEADS * HEAD, D), preferred_element_type=jnp.float32).astype(jnp.bfloat16)
    return (attended, block_out)
```

```python
import functools

import jax
import jax.numpy as jnp
from jax import lax
from jax.experimental import pallas as pl
from jax.experimental.pallas import tpu as pltpu
from jax.sharding import PartitionSpec as P

RESP = 5
PROMPT_MIN = 512
MESH = pl.DeviceIdType.MESH
LOW = -1e30
CHUNKS = 4

rope_base = 500000.0


def first_slots(owner, counts):
    order = jnp.arange(owner.shape[0], dtype=jnp.int32)
    earlier = (owner[:, None] == owner[None, :]) & (order[None, :] < order[:, None])
    return jnp.sum(jnp.where(earlier, counts[None, :], 0), axis=1)


def nt(a, b):
    return lax.dot_general(a, b, (((1,), (1,)), ((), ())), preferred_element_type=jnp.float32)


def nn(a, b):
    return jnp.dot(a, b, preferred_element_type=jnp.float32)


def kernel(
    cfg,
    hidden_hbm, gain_ref, kvw_hbm, q_ref, new_ref, cache_hbm, ow_hbm,
    cos_ref, sin_ref, target_ref, window_ref, row_code_ref, col_code_ref, pos_ref,
    attended_ref, block_ref,
    hidden, kvw, cache, ow, ow_far, normed, acc, keys, values, q_all,
    mix_all, stat_all, mix_mine, stat_mine, scores, cache_mix, att_rows, att_flat, att_all,
    local_sem, cache_sem, q_send, q_recv, mix_send, mix_recv, stat_send, stat_recv,
    att_send, att_recv, ow_send, ow_recv,
):
    n, roles, slots, heads, local_heads, context, head, used, padded = cfg
    group = heads // local_heads
    per = n // roles
    rows = slots * heads
    scale = head ** (-0.5)
    me = lax.axis_index("dev")
    role = lax.axis_index("role")
    width = hidden.shape[1]
    step = width // CHUNKS
    span = cache.shape[0] // CHUNKS

    hidden_copy = pltpu.make_async_copy(hidden_hbm, hidden, local_sem.at[CHUNKS])
    hidden_copy.start()
    kvw_copies = []
    for c in range(CHUNKS):
        part = pl.ds(c * step, step)
        kvw_copies.append(pltpu.make_async_copy(kvw_hbm.at[part], kvw.at[part], local_sem.at[c]))
        kvw_copies[-1].start()
    ow_copy = pltpu.make_async_copy(ow_hbm, ow, local_sem.at[CHUNKS + 1])
    ow_copy.start()
    cache_copies = []
    for c in range(CHUNKS):
        part = pl.ds(c * span, span)
        cache_copies.append(
            pltpu.make_async_copy(cache_hbm.at[part], cache.at[part], cache_sem.at[c])
        )
        cache_copies[-1].start()

    barrier = pltpu.get_barrier_semaphore()

    def greet(i, carry):
        other = lax.rem(me * roles + role + i, n * roles)
        pl.semaphore_signal(
            barrier,
            inc=1,
            device_id={"dev": other // roles, "role": lax.rem(other, roles)},
            device_id_type=MESH,
        )
        return carry

    lax.fori_loop(1, n * roles, greet, 0)
    pl.semaphore_wait(barrier, n * roles - 1)

    def q_copy(peer, slot):
        return pltpu.make_async_remote_copy(
            src_ref=q_ref, dst_ref=q_all.at[slot], send_sem=q_send.at[peer],
            recv_sem=q_recv.at[slot], device_id={"dev": peer}, device_id_type=MESH,
        )

    def mix_copy(peer, slot):
        return pltpu.make_async_remote_copy(
            src_ref=mix_mine, dst_ref=mix_all.at[slot, pl.ds(0, used)], send_sem=mix_send.at[peer],
            recv_sem=mix_recv.at[slot], device_id={"dev": peer}, device_id_type=MESH,
        )

    def stat_copy(peer, slot):
        return pltpu.make_async_remote_copy(
            src_ref=stat_mine, dst_ref=stat_all.at[slot], send_sem=stat_send.at[peer],
            recv_sem=stat_recv.at[slot], device_id={"dev": peer}, device_id_type=MESH,
        )

    def every(action):
        def body(o, carry):
            action(lax.rem(me + o, n))
            return carry

        lax.fori_loop(1, n, body, 0)

    every(lambda peer: q_copy(peer, me).start())
    q_all[me] = q_ref[...]

    def ow_far_copy(j):
        return pltpu.make_async_remote_copy(
            src_ref=ow_hbm, dst_ref=ow_far.at[j - 1], send_sem=ow_send.at[j - 1],
            recv_sem=ow_recv.at[j - 1],
            device_id={"role": lax.rem(role + roles - j, roles)}, device_id_type=MESH,
        )

    for j in range(1, roles):
        ow_far_copy(j).start()

    for e in range(n):
        mix_all[e, used:padded, :] = jnp.zeros((padded - used, head), jnp.bfloat16)

    hidden_copy.wait()
    block = 32

    def normalise(i, carry):
        part = pl.ds(pl.multiple_of(i * block, block), block)
        x = hidden[part, :].astype(jnp.float32)
        ratio = lax.rsqrt(jnp.mean(x * x, axis=-1, keepdims=True) + 1e-05)
        normed[part, :] = (x * ratio * gain_ref[...]).astype(jnp.bfloat16)
        return carry

    lax.fori_loop(0, hidden.shape[0] // block, normalise, 0)
    for c in range(CHUNKS):
        kvw_copies[c].wait()
        part = slice(c * step, (c + 1) * step)
        product = nn(normed[:, part], kvw[part, :])
        if c == 0:
            acc[...] = product
        else:
            acc[...] += product
    for k in range(local_heads):
        raw = acc[:, 2 * k * head : (2 * k + 1) * head]
        turned = jnp.concatenate([raw[:, head // 2 :], raw[:, : head // 2]], axis=1)
        keys[k] = (raw * cos_ref[...] + turned * sin_ref[...]).astype(jnp.bfloat16)
        values[k] = acc[:, (2 * k + 1) * head : (2 * k + 2) * head].astype(jnp.bfloat16)

    every(lambda peer: q_copy(peer, peer).wait_recv())
    target = target_ref[...]
    column = lax.broadcasted_iota(jnp.int32, (used, rows), 1)
    chosen = jnp.concatenate(
        [(target[:, :1] - e * rows == column).astype(jnp.float32) for e in range(n)], axis=1
    ).astype(jnp.bfloat16)
    table = nn(chosen, q_all[...].reshape(n * rows, head)).astype(jnp.bfloat16)
    share = used // local_heads
    peaks, totals, mixes = [], [], []
    for k in range(local_heads):
        mine = slice(k * share, (k + 1) * share)
        valid = target[mine, 1:2] == window_ref[0:1, :]
        s = jnp.where(valid, nt(table[mine], keys[k]) * scale, LOW)
        peak = jnp.max(s, axis=1, keepdims=True)
        w = jnp.where(valid, jnp.exp(s - peak), 0.0)
        peaks.append(peak)
        totals.append(jnp.sum(w, axis=1, keepdims=True))
        mixes.append(nn(w.astype(jnp.bfloat16), values[k]))
    mix_mine[...] = jnp.concatenate(mixes, axis=0).astype(jnp.bfloat16)
    lane = lax.broadcasted_iota(jnp.int32, (used, padded), 1)
    stats = jnp.where(
        lane == 0, jnp.concatenate(peaks, axis=0), jnp.where(lane == 1, jnp.concatenate(totals, axis=0), 0.0)
    )
    stats = jnp.concatenate([stats, jnp.zeros((padded - used, padded), jnp.float32)], axis=0)
    stat_mine[...] = stats.T[:8]

    def send_state(peer):
        stat_copy(peer, me).start()
        mix_copy(peer, me).start()

    every(send_state)
    mix_all[me, 0:used, :] = mix_mine[...]
    stat_all[me] = stat_mine[...]

    for c in range(CHUNKS):
        cache_copies[c].wait()
    line = 2 * local_heads * context

    def score(s, carry):
        part = pl.ds(pl.multiple_of(s * heads, heads), heads)
        block_rows = pl.ds(pl.multiple_of(s * line, line), line)
        scores[part, :] = nt(q_ref[part, :], cache[block_rows, :]) * scale
        return carry

    lax.fori_loop(0, slots, score, 0, unroll=4)
    col = lax.broadcasted_iota(jnp.int32, (rows, line), 1)
    row = lax.broadcasted_iota(jnp.int32, (rows, line), 0)
    own_head = lax.rem(row, heads) // group
    valid = (lax.rem(col, 2 * local_heads) == 2 * own_head) & (
        col // (2 * local_heads) < pos_ref[:, :1]
    )
    s = jnp.where(valid, scores[...], LOW)
    cache_peak = jnp.max(s, axis=1, keepdims=True)
    w = jnp.where(valid, jnp.exp(s - cache_peak), 0.0)
    cache_total = jnp.sum(w, axis=1, keepdims=True)
    scores[...] = pltpu.roll(w, 1, 1)

    def mix(s, carry):
        part = pl.ds(pl.multiple_of(s * heads, heads), heads)
        block_rows = pl.ds(pl.multiple_of(s * line, line), line)
        cache_mix[part, :] = nn(scores[part, :].astype(jnp.bfloat16), cache[block_rows, :])
        return carry

    lax.fori_loop(0, slots, mix, 0, unroll=4)

    fresh = new_ref[...]
    near = nt(q_ref[...], fresh) * scale
    fcol = lax.broadcasted_iota(jnp.int32, near.shape, 1)
    frow = lax.broadcasted_iota(jnp.int32, near.shape, 0)
    pair = 2 * (frow // group)
    self_score = jnp.max(jnp.where(fcol == pair, near, LOW), axis=1, keepdims=True)

    def wait_state(peer):
        stat_copy(peer, peer).wait_recv()
        mix_copy(peer, peer).wait_recv()

    every(wait_state)
    row_code = row_code_ref[:, :1]
    held = jnp.concatenate(
        [jnp.where(row_code == col_code_ref[e : e + 1, :], stat_all[e, 0:1, :], LOW) for e in range(n)],
        axis=1,
    )
    totals_all = jnp.concatenate([stat_all[e, 1:2, :] for e in range(n)], axis=1)
    peak = jnp.maximum(jnp.maximum(cache_peak, self_score), jnp.max(held, axis=1, keepdims=True))
    weight = jnp.where(held > 0.5 * LOW, jnp.exp(held - peak), 0.0)
    total = jnp.sum(weight * totals_all, axis=1, keepdims=True)
    mixed = nn(weight.astype(jnp.bfloat16), mix_all[...].reshape(n * padded, head))
    cache_weight = jnp.exp(cache_peak - peak)
    self_weight = jnp.exp(self_score - peak)
    total = total + cache_total * cache_weight + self_weight
    mixed = mixed + cache_mix[...] * cache_weight
    mixed = mixed + nn(jnp.where(fcol == pair + 1, self_weight, 0.0).astype(jnp.bfloat16), fresh)
    att = mixed / total
    att_rows[...] = att
    attended_ref[...] = att.astype(jnp.bfloat16)
    for h in range(heads):
        att_flat[:, h * head : (h + 1) * head] = att_rows[pl.ds(h, slots, stride=heads), :].astype(
            jnp.bfloat16
        )

    home = me // per
    place = lax.rem(me, per)

    def att_copy(peer, peer_role, from_role, slot):
        return pltpu.make_async_remote_copy(
            src_ref=att_flat, dst_ref=att_all.at[from_role, slot], send_sem=att_send.at[peer],
            recv_sem=att_recv.at[from_role, slot],
            device_id={"dev": peer, "role": peer_role}, device_id_type=MESH,
        )

    every(lambda peer: att_copy(peer, home, role, place).start())

    @pl.when(home != role)
    def _():
        att_copy(me, home, role, place).start()

    @pl.when(home == role)
    def _():
        att_all[role, place] = att_flat[...]

    for j in range(1, roles):
        ow_far_copy(j).wait()
    ow_copy.wait()

    def wait_att(i, carry):
        from_role = i // per
        slot = lax.rem(i, per)

        @pl.when(jnp.logical_not((from_role == role) & (role * per + slot == me)))
        def _():
            att_copy(me, role, from_role, slot).wait_recv()

        return carry

    lax.fori_loop(0, n, wait_att, 0)
    out = nn(att_all[role].reshape(per * slots, heads * head), ow[...])
    for j in range(1, roles):
        far = lax.rem(role + j, roles)
        out = out + nn(att_all[far].reshape(per * slots, heads * head), ow_far[j - 1])
    block_ref[...] = out.astype(jnp.bfloat16)

    every(lambda peer: q_copy(peer, me).wait_send())

    def sent_state(peer):
        stat_copy(peer, me).wait_send()
        mix_copy(peer, me).wait_send()

    every(sent_state)
    every(lambda peer: att_copy(peer, home, role, place).wait_send())

    @pl.when(home != role)
    def _():
        att_copy(me, home, role, place).wait_send()


def on_device(
    prompt_hidden,
    norm_gain,
    kv_weight,
    prompt_excess,
    prompt_owner,
    response_counts,
    queries,
    new_kv,
    response_cache,
    positions,
    out_weight,
):
    n = lax.axis_size("dev")
    roles = lax.axis_size("role")
    device = lax.axis_index("dev")
    rows, width = prompt_hidden.shape
    local_heads = kv_weight.shape[1]
    head = kv_weight.shape[3]
    slots, heads, _ = queries.shape
    group = heads // local_heads
    context = response_cache.shape[1]
    prompts = prompt_excess.shape[0]
    columns = out_weight.shape[2]
    reach = min(rows // PROMPT_MIN + 2, prompts)
    used = reach * RESP * heads
    padded = -(-used // 128) * 128
    i32 = jnp.int32

    lengths = PROMPT_MIN + prompt_excess
    upto = jnp.arange(prompts, dtype=i32)
    ends = jnp.sum(jnp.where(upto[None, :] <= upto[:, None], lengths[None, :], 0), axis=1)
    starts = ends - lengths
    tokens = device * rows + jnp.arange(rows, dtype=i32)
    prompt_id = jnp.sum((tokens[:, None] >= ends[None, :]).astype(i32), axis=1)
    member = prompt_id[:, None] == upto[None, :]
    offsets = tokens - jnp.sum(jnp.where(member, starts[None, :], 0), axis=1)
    lanes = jnp.arange(head, dtype=i32)
    half = head // 2
    freq = rope_base ** (-(lanes % half).astype(jnp.float32) * 2.0 / head)
    angles = offsets.astype(jnp.float32)[:, None] * freq[None, :]
    cosine = jnp.cos(angles)
    sine = jnp.where(lanes[None, :] < half, -1.0, 1.0) * jnp.sin(angles)

    all_first = jnp.sum((jnp.arange(n, dtype=i32)[:, None] * rows >= ends[None, :]).astype(i32), axis=1)
    first_prompt = jnp.sum((device * rows >= ends).astype(i32))
    window = jnp.broadcast_to((prompt_id - first_prompt)[None, :], (8, rows))

    first = first_slots(prompt_owner, response_counts)
    j = jnp.arange(padded, dtype=i32)
    share = reach * RESP * group
    k_of = j // share
    w_of = (j % share) // (RESP * group)
    r_of = (j % (RESP * group)) // group
    h_of = k_of * group + j % group
    inside = j < used
    p_of = first_prompt + w_of
    at = p_of[:used, None] == upto[None, :]
    seat = jnp.sum(jnp.where(at, (prompt_owner * slots + first)[None, :], 0), axis=1)
    count = jnp.sum(jnp.where(at, response_counts[None, :], 0), axis=1)
    live = r_of[:used] < count
    target = jnp.where(live, (seat + r_of[:used]) * heads + h_of[:used], -1)
    seen = jnp.where(live, w_of[:used], -1)
    target = jnp.where(jnp.arange(128, dtype=i32)[None, :] == 1, seen[:, None], target[:, None])

    col_code = ((all_first[:, None] + w_of[None, :]) * RESP + r_of[None, :]) * heads + h_of[None, :]
    col_code = jnp.where(inside[None, :], col_code, -2)

    rix = jnp.arange(slots * heads, dtype=i32)
    slot = rix // heads
    match = (
        (prompt_owner[None, :] == device)
        & (first[None, :] <= slot[:, None])
        & (slot[:, None] < (first + response_counts)[None, :])
    )
    entry = jnp.sum(
        jnp.where(match, upto[None, :] * RESP + slot[:, None] - first[None, :], 0), axis=1
    )
    row_code = jnp.where(jnp.any(match, axis=1), entry * heads + rix % heads, -1)
    row_code = jnp.broadcast_to(row_code[:, None], (slots * heads, 128))
    pos = jnp.broadcast_to(positions[:, None, None], (slots, heads, 128)).reshape(slots * heads, 128)

    line = 2 * local_heads * context
    bf16, f32 = jnp.bfloat16, jnp.float32
    dma = pltpu.SemaphoreType.DMA
    anywhere = pl.BlockSpec(memory_space=pl.ANY)
    vmem = pl.BlockSpec(memory_space=pltpu.VMEM)
    cfg = (n, roles, slots, heads, local_heads, context, head, used, padded)
    attended, block_out = pl.pallas_call(
        functools.partial(kernel, cfg),
        out_shape=(
            jax.ShapeDtypeStruct((slots * heads, head), bf16),
            jax.ShapeDtypeStruct((n // roles * slots, columns), bf16),
        ),
        in_specs=[anywhere, vmem, anywhere, vmem, vmem, anywhere, anywhere] + [vmem] * 7,
        out_specs=(vmem, vmem),
        scratch_shapes=[
            pltpu.VMEM((rows, width), bf16),
            pltpu.VMEM((width, local_heads * 2 * head), bf16),
            pltpu.VMEM((slots * line, head), bf16),
            pltpu.VMEM((heads * head, columns), bf16),
            pltpu.VMEM((roles - 1, heads * head, columns), bf16),
            pltpu.VMEM((rows, width), bf16),
            pltpu.VMEM((rows, local_heads * 2 * head), f32),
            pltpu.VMEM((local_heads, rows, head), bf16),
            pltpu.VMEM((local_heads, rows, head), bf16),
            pltpu.VMEM((n, slots * heads, head), bf16),
            pltpu.VMEM((n, padded, head), bf16),
            pltpu.VMEM((n, 8, padded), f32),
            pltpu.VMEM((used, head), bf16),
            pltpu.VMEM((8, padded), f32),
            pltpu.VMEM((slots * heads, line), f32),
            pltpu.VMEM((slots * heads, head), f32),
            pltpu.VMEM((slots * heads, head), f32),
            pltpu.VMEM((slots, heads * head), bf16),
            pltpu.VMEM((roles, n // roles, slots, heads * head), bf16),
            dma((CHUNKS + 2,)),
            dma((CHUNKS,)),
            dma((n,)),
            dma((n,)),
            dma((n,)),
            dma((n,)),
            dma((n,)),
            dma((n,)),
            dma((n,)),
            dma((roles, n // roles)),
            dma((roles - 1,)),
            dma((roles - 1,)),
        ],
        compiler_params=pltpu.CompilerParams(
            collective_id=0, has_side_effects=True, vmem_limit_bytes=56 * 1024 * 1024
        ),
    )(
        prompt_hidden,
        norm_gain.reshape(1, width),
        kv_weight.reshape(width, local_heads * 2 * head),
        queries.reshape(slots * heads, head),
        new_kv.reshape(slots * local_heads * 2, head),
        response_cache.reshape(slots * line, head),
        out_weight.reshape(heads * head, columns),
        cosine,
        sine,
        target,
        window,
        row_code,
        col_code,
        pos,
    )
    return (attended.reshape(slots, heads, head), block_out)


def solution(mesh):
    return jax.shard_map(
        on_device,
        mesh=mesh,
        in_specs=(
            P(("groups", "dev"), None),
            P(),
            P(None, "role", None, None),
            P("groups"),
            P("groups"),
            P("groups"),
            P(("groups", "dev"), "role", None),
            P(("groups", "dev"), "role", None, None),
            P(("groups", "dev"), None, "role", None, None),
            P(("groups", "dev")),
            P("role", None, "dev"),
        ),
        out_specs=(P(("groups", "dev"), "role", None), P(("groups", "role"), "dev")),
        check_vma=False,
    )
```

```python
import functools

import jax
import jax.numpy as jnp
from jax import lax
from jax.experimental import pallas as pl
from jax.experimental.pallas import tpu as pltpu
from jax.sharding import PartitionSpec as P

RESP = 5
PROMPT_MIN = 512
MESH = pl.DeviceIdType.MESH
LOW = -1e30
CHUNKS = 4

rope_base = 500000.0


def nt(a, b):
    return lax.dot_general(a, b, (((1,), (1,)), ((), ())), preferred_element_type=jnp.float32)


def nn(a, b):
    return jnp.dot(a, b, preferred_element_type=jnp.float32)


def kernel(
    cfg,
    hidden_hbm, gain_ref, kvw_hbm, q_ref, new_ref, cache_hbm, ow_hbm,
    freq_ref, excess_ref, owner_ref, count_ref, pos_ref,
    attended_ref, block_ref,
    hidden, kvx, wide, kvw, cos_ref, sin_ref, cache, ow, ow_far, normed, acc, keys, values, q_all,
    mix_all, stat_all, mix_mine, stat_mine, scores, cache_mix, att_rows, att_flat, att_all,
    local_sem, cache_sem, q_send, q_recv, mix_send, mix_recv, stat_send, stat_recv,
    att_send, att_pass, att_recv, ow_send, ow_recv,
):
    n, inner, roles, slots, heads, local_heads, context, head, reach, used, padded = cfg
    outer = n // inner
    group = heads // local_heads
    per = n // roles
    rows = slots * heads
    scale = head ** (-0.5)
    me = lax.axis_index("dev")
    role = lax.axis_index("role")
    width = hidden.shape[1]
    step = width // CHUNKS
    pairs = 2 * local_heads
    tokens = hidden.shape[0]
    prompts = excess_ref.shape[0]
    i32 = jnp.int32
    major, minor = me // inner, lax.rem(me, inner)
    span = cache.shape[0] // CHUNKS

    hidden_copy = pltpu.make_async_copy(hidden_hbm, hidden, local_sem.at[CHUNKS])
    hidden_copy.start()
    kvw_copies = []
    for c in range(CHUNKS):
        part = pl.ds(c * step * pairs, step * pairs)
        kvw_copies.append(pltpu.make_async_copy(kvw_hbm.at[part], kvx.at[part], local_sem.at[c]))
        kvw_copies[-1].start()
    ow_copy = pltpu.make_async_copy(ow_hbm, ow, local_sem.at[CHUNKS + 1])
    ow_copy.start()
    cache_copies = []
    for c in range(CHUNKS):
        part = pl.ds(c * span, span)
        cache_copies.append(
            pltpu.make_async_copy(cache_hbm.at[part], cache.at[part], cache_sem.at[c])
        )
        cache_copies[-1].start()

    barrier = pltpu.get_barrier_semaphore()

    def greet(i, carry):
        other = lax.rem(me * roles + role + i, n * roles)
        pl.semaphore_signal(
            barrier,
            inc=1,
            device_id={"dev": other // roles, "role": lax.rem(other, roles)},
            device_id_type=MESH,
        )
        return carry

    lax.fori_loop(1, n * roles, greet, 0)

    lengths = [PROMPT_MIN + excess_ref[p] for p in range(prompts)]
    ends = [lengths[0]]
    for p in range(1, prompts):
        ends.append(ends[-1] + lengths[p])
    owners = [owner_ref[p] for p in range(prompts)]
    counts = [count_ref[p] for p in range(prompts)]
    firsts = []
    for p in range(prompts):
        first = jnp.int32(0)
        for q in range(p):
            first = first + jnp.where(owners[q] == owners[p], counts[q], 0)
        firsts.append(first)

    def prompt_of(token):
        found = jnp.zeros_like(token)
        for p in range(prompts):
            found = found + jnp.where(token >= ends[p], 1, 0)
        return found

    def reply_of(index):
        k = jnp.zeros_like(index)
        for m in range(1, local_heads):
            k = k + jnp.where(index >= m * (used // local_heads), 1, 0)
        rest = index - k * (used // local_heads)
        w = jnp.zeros_like(index)
        for m in range(1, reach):
            w = w + jnp.where(rest >= m * RESP * group, 1, 0)
        rest = rest - w * (RESP * group)
        return w, lax.div(rest, group), k * group + lax.rem(rest, group)

    first_prompt = prompt_of(me * tokens)
    w_of, r_of, h_of = reply_of(lax.broadcasted_iota(i32, (used, 128), 0))
    seat = jnp.zeros_like(w_of)
    number = jnp.zeros_like(w_of)
    for p in range(prompts):
        here = first_prompt + w_of == p
        seat = jnp.where(here, owners[p] * slots + firsts[p], seat)
        number = jnp.where(here, counts[p], number)
    live = r_of < number
    target = jnp.where(live, (seat + r_of) * heads + h_of, -1)
    seen = jnp.where(live, w_of, -1)
    window = prompt_of(me * tokens + lax.broadcasted_iota(i32, (8, tokens), 1)) - first_prompt
    col_first = prompt_of(tokens * lax.broadcasted_iota(i32, (n, padded), 0))
    col_index = lax.broadcasted_iota(i32, (n, padded), 1)
    cw, cr, ch = reply_of(col_index)
    col_code = jnp.where(col_index < used, ((col_first + cw) * RESP + cr) * heads + ch, -2)
    row_index = lax.broadcasted_iota(i32, (rows, 128), 0)
    row_slot = lax.div(row_index, heads)
    row_code = jnp.full((rows, 128), -1, i32)
    for p in range(prompts):
        rank = row_slot - firsts[p]
        mine = (owners[p] == me) & (rank >= 0) & (rank < counts[p])
        row_code = jnp.where(mine, (p * RESP + rank) * heads + lax.rem(row_index, heads), row_code)

    half = head // 2
    token = me * tokens + lax.broadcasted_iota(i32, (tokens, head), 0)
    offset = token
    for p in range(prompts):
        offset = offset - jnp.where(token >= ends[p], lengths[p], 0)
    angle = offset.astype(jnp.float32) * freq_ref[...]
    cos_ref[...] = jnp.cos(angle)
    lane = lax.broadcasted_iota(i32, (tokens, head), 1)
    sine = jnp.sin(angle)
    sin_ref[...] = jnp.where(lane < half, -sine, sine)
    for e in range(n):
        mix_all[e, used:padded, :] = jnp.zeros((padded - used, head), jnp.bfloat16)

    pl.semaphore_wait(barrier, n * roles - 1)

    def peer_at(o, i):
        return lax.rem(major + o, outer) * inner + lax.rem(minor + i, inner)

    class Gather:
        def __init__(self, mine, everyone, send, recv):
            self.refs = mine, everyone, send, recv

        def copy(self, src, slot, o, i, peer):
            mine, everyone, send, recv = self.refs
            return pltpu.make_async_remote_copy(
                src_ref=src, dst_ref=everyone(slot), send_sem=send.at[o, i],
                recv_sem=recv.at[slot], device_id={"dev": peer}, device_id_type=MESH,
            )

        def own(self, o, i):
            return self.copy(self.refs[0], me, o, i, peer_at(o, i))

        def passed(self, o, i):
            slot = peer_at(o, 0)
            return self.copy(self.refs[1](slot), slot, o, i, peer_at(0, i))

        def start(self):
            for o in range(1, outer):
                self.own(o, 0).start()
            for i in range(1, inner):
                self.own(0, i).start()

        def forward(self):
            for o in range(1, outer):
                self.passed(o, 0).wait_recv()
                for i in range(1, inner):
                    self.passed(o, i).start()

        def finish(self):
            for o in range(outer):
                for i in range(1, inner):
                    slot = peer_at(o, i)
                    self.copy(self.refs[0], slot, 0, 0, me).wait_recv()

        def sent(self):
            for o in range(1, outer):
                self.own(o, 0).wait_send()
                for i in range(1, inner):
                    self.passed(o, i).wait_send()
            for i in range(1, inner):
                self.own(0, i).wait_send()

    q_net = Gather(q_ref, lambda e: q_all.at[e], q_send, q_recv)
    mix_net = Gather(mix_mine, lambda e: mix_all.at[e, pl.ds(0, used)], mix_send, mix_recv)
    stat_net = Gather(stat_mine, lambda e: stat_all.at[e], stat_send, stat_recv)
    q_net.start()
    q_all[me] = q_ref[...]

    def ow_far_copy(j):
        return pltpu.make_async_remote_copy(
            src_ref=ow_hbm, dst_ref=ow_far.at[j - 1], send_sem=ow_send.at[j - 1],
            recv_sem=ow_recv.at[j - 1],
            device_id={"role": lax.rem(role + roles - j, roles)}, device_id_type=MESH,
        )

    for j in range(1, roles):
        ow_far_copy(j).start()

    hidden_copy.wait()
    block = 32

    def normalise(i, carry):
        part = pl.ds(pl.multiple_of(i * block, block), block)
        x = hidden[part, :].astype(jnp.float32)
        ratio = lax.rsqrt(jnp.mean(x * x, axis=-1, keepdims=True) + 1e-05)
        normed[part, :] = (x * ratio * gain_ref[...]).astype(jnp.bfloat16)
        return carry

    lax.fori_loop(0, hidden.shape[0] // block, normalise, 0)
    tall = wide.shape[1]

    def unweave(i, carry):
        lot = lax.rem(i, 2)
        wide[lot] = kvx[pl.ds(pl.multiple_of(i * tall, tall), tall), :].astype(jnp.float32)
        part = pl.ds(pl.multiple_of(i * (tall // pairs), tall // pairs), tall // pairs)
        for m in range(pairs):
            kvw[part, m * head : (m + 1) * head] = wide[
                lot, pl.ds(m, tall // pairs, stride=pairs), :
            ].astype(jnp.bfloat16)
        return carry

    per_chunk = step * pairs // tall
    for c in range(CHUNKS):
        kvw_copies[c].wait()
        lax.fori_loop(c * per_chunk, (c + 1) * per_chunk, unweave, 0, unroll=2)
        if c == 0:
            q_net.forward()
        part = slice(c * step, (c + 1) * step)
        product = nn(normed[:, part], kvw[part, :])
        if c == 0:
            acc[...] = product
        else:
            acc[...] += product
    for k in range(local_heads):
        raw = acc[:, 2 * k * head : (2 * k + 1) * head]
        turned = jnp.concatenate([raw[:, head // 2 :], raw[:, : head // 2]], axis=1)
        keys[k] = (raw * cos_ref[...] + turned * sin_ref[...]).astype(jnp.bfloat16)
        values[k] = acc[:, (2 * k + 1) * head : (2 * k + 2) * head].astype(jnp.bfloat16)

    q_net.finish()
    column = lax.broadcasted_iota(jnp.int32, (used, rows), 1)
    chosen = jnp.concatenate(
        [(target[:, :1] - e * rows == column).astype(jnp.float32) for e in range(n)], axis=1
    ).astype(jnp.bfloat16)
    table = nn(chosen, q_all[...].reshape(n * rows, head)).astype(jnp.bfloat16)
    share = used // local_heads
    peaks, totals, mixes = [], [], []
    for k in range(local_heads):
        mine = slice(k * share, (k + 1) * share)
        valid = seen[mine, :1] == window[0:1, :]
        s = jnp.where(valid, nt(table[mine], keys[k]) * scale, LOW)
        peak = jnp.max(s, axis=1, keepdims=True)
        w = jnp.where(valid, jnp.exp(s - peak), 0.0)
        peaks.append(peak)
        totals.append(jnp.sum(w, axis=1, keepdims=True))
        mixes.append(nn(w.astype(jnp.bfloat16), values[k]))
    mix_mine[...] = jnp.concatenate(mixes, axis=0).astype(jnp.bfloat16)
    lane = lax.broadcasted_iota(jnp.int32, (used, padded), 1)
    stats = jnp.where(
        lane == 0, jnp.concatenate(peaks, axis=0), jnp.where(lane == 1, jnp.concatenate(totals, axis=0), 0.0)
    )
    stats = jnp.concatenate([stats, jnp.zeros((padded - used, padded), jnp.float32)], axis=0)
    stat_mine[...] = stats.T[:8]

    stat_net.start()
    mix_net.start()
    mix_all[me, 0:used, :] = mix_mine[...]
    stat_all[me] = stat_mine[...]

    for c in range(CHUNKS):
        cache_copies[c].wait()
    line = 2 * local_heads * context

    def score(s, carry):
        part = pl.ds(pl.multiple_of(s * heads, heads), heads)
        block_rows = pl.ds(pl.multiple_of(s * line, line), line)
        raw = nt(q_ref[part, :], cache[block_rows, :]) * scale
        held_here = lax.div(col, pairs) < pos_ref[s]
        scores[part, :] = jnp.where((lax.rem(col, pairs) == 2 * own_head) & held_here, raw, LOW)
        return carry

    col = lax.broadcasted_iota(i32, (heads, line), 1)
    own_head = lax.div(lax.broadcasted_iota(i32, (heads, line), 0), group)

    lax.fori_loop(0, slots, score, 0, unroll=4)
    stat_net.forward()
    mix_net.forward()
    s = scores[...]
    cache_peak = jnp.max(s, axis=1, keepdims=True)
    w = jnp.where(s > 0.5 * LOW, jnp.exp(s - cache_peak), 0.0)
    cache_total = jnp.sum(w, axis=1, keepdims=True)
    scores[...] = pltpu.roll(w, 1, 1)

    def mix(s, carry):
        part = pl.ds(pl.multiple_of(s * heads, heads), heads)
        block_rows = pl.ds(pl.multiple_of(s * line, line), line)
        cache_mix[part, :] = nn(scores[part, :].astype(jnp.bfloat16), cache[block_rows, :])
        return carry

    lax.fori_loop(0, slots, mix, 0, unroll=4)

    fresh = new_ref[...]
    near = nt(q_ref[...], fresh) * scale
    fcol = lax.broadcasted_iota(jnp.int32, near.shape, 1)
    frow = lax.broadcasted_iota(jnp.int32, near.shape, 0)
    pair = 2 * (frow // group)
    self_score = jnp.max(jnp.where(fcol == pair, near, LOW), axis=1, keepdims=True)

    stat_net.finish()
    mix_net.finish()
    row_code = row_code[:, :1]
    held = jnp.concatenate(
        [jnp.where(row_code == col_code[e : e + 1, :], stat_all[e, 0:1, :], LOW) for e in range(n)],
        axis=1,
    )
    totals_all = jnp.concatenate([stat_all[e, 1:2, :] for e in range(n)], axis=1)
    peak = jnp.maximum(jnp.maximum(cache_peak, self_score), jnp.max(held, axis=1, keepdims=True))
    weight = jnp.where(held > 0.5 * LOW, jnp.exp(held - peak), 0.0)
    total = jnp.sum(weight * totals_all, axis=1, keepdims=True)
    mixed = nn(weight.astype(jnp.bfloat16), mix_all[...].reshape(n * padded, head))
    cache_weight = jnp.exp(cache_peak - peak)
    self_weight = jnp.exp(self_score - peak)
    total = total + cache_total * cache_weight + self_weight
    mixed = mixed + cache_mix[...] * cache_weight
    mixed = mixed + nn(jnp.where(fcol == pair + 1, self_weight, 0.0).astype(jnp.bfloat16), fresh)
    att = mixed / total
    att_rows[...] = att
    attended_ref[...] = att.astype(jnp.bfloat16)
    for h in range(heads):
        att_flat[:, h * head : (h + 1) * head] = att_rows[pl.ds(h, slots, stride=heads), :].astype(
            jnp.bfloat16
        )

    home = me // per
    place = lax.rem(me, per)

    fold = outer // roles

    def att_copy(src, from_role, o, slot, sem, peer, peer_role):
        return pltpu.make_async_remote_copy(
            src_ref=src, dst_ref=att_all.at[from_role, slot], send_sem=sem,
            recv_sem=att_recv.at[from_role, slot],
            device_id={"dev": peer, "role": peer_role}, device_id_type=MESH,
        )

    def att_own(o, i):
        return att_copy(att_flat, role, o, place, att_send.at[o, i], peer_at(o, i), home)

    def att_passed(from_role, o, i):
        slot = o * inner + minor
        return att_copy(
            att_all.at[from_role, slot], from_role, o, slot,
            att_pass.at[from_role, o, i], peer_at(0, i), role,
        )

    for o in range(1, outer):
        att_own(o, 0).start()
    for i in range(1, inner):
        att_own(0, i).start()

    @pl.when(home != role)
    def _():
        att_own(0, 0).start()

    @pl.when(home == role)
    def _():
        att_all[role, place] = att_flat[...]

    for j in range(1, roles):
        ow_far_copy(j).wait()
    ow_copy.wait()

    for o in range(fold):
        for from_role in range(roles):

            @pl.when(role * fold + o != major)
            def _():
                att_passed(from_role, o, 0).wait_recv()
                for i in range(1, inner):
                    att_passed(from_role, o, i).start()

            @pl.when((role * fold + o == major) & (from_role != role))
            def _():
                att_passed(from_role, o, 0).wait_recv()

    for o in range(fold):
        for from_role in range(roles):
            for i in range(1, inner):
                slot = o * inner + lax.rem(minor + i, inner)
                att_copy(att_flat, from_role, o, slot, att_send.at[0, 0], me, role).wait_recv()

    out = nn(att_all[role].reshape(per * slots, heads * head), ow[...])
    for j in range(1, roles):
        far = lax.rem(role + j, roles)
        out = out + nn(att_all[far].reshape(per * slots, heads * head), ow_far[j - 1])
    block_ref[...] = out.astype(jnp.bfloat16)

    q_net.sent()
    stat_net.sent()
    mix_net.sent()
    for o in range(1, outer):
        att_own(o, 0).wait_send()
    for i in range(1, inner):
        att_own(0, i).wait_send()

    @pl.when(home != role)
    def _():
        att_own(0, 0).wait_send()

    for o in range(fold):

        @pl.when(role * fold + o != major)
        def _():
            for from_role in range(roles):
                for i in range(1, inner):
                    att_passed(from_role, o, i).wait_send()


def on_device(
    prompt_hidden,
    norm_gain,
    kv_weight,
    prompt_excess,
    prompt_owner,
    response_counts,
    queries,
    new_kv,
    response_cache,
    positions,
    out_weight,
):
    n = lax.axis_size("dev")
    roles = lax.axis_size("role")
    rows, width = prompt_hidden.shape
    local_heads = kv_weight.shape[1]
    head = kv_weight.shape[3]
    slots, heads, _ = queries.shape
    group = heads // local_heads
    context = response_cache.shape[1]
    prompts = prompt_excess.shape[0]
    columns = out_weight.shape[2]
    reach = min(rows // PROMPT_MIN + 2, prompts)
    used = reach * RESP * heads
    padded = -(-used // 128) * 128
    inner = 1
    while inner * inner < n:
        inner *= 2
    half = head // 2
    freq = rope_base ** (-jnp.arange(half, dtype=jnp.float32) * 2.0 / head)
    freq = jnp.concatenate([freq, freq])[None, :]
    line = 2 * local_heads * context
    bf16, f32 = jnp.bfloat16, jnp.float32
    dma = pltpu.SemaphoreType.DMA
    anywhere = pl.BlockSpec(memory_space=pl.ANY)
    vmem = pl.BlockSpec(memory_space=pltpu.VMEM)
    smem = pl.BlockSpec(memory_space=pltpu.SMEM)
    cfg = (n, inner, roles, slots, heads, local_heads, context, head, reach, used, padded)
    attended, block_out = pl.pallas_call(
        functools.partial(kernel, cfg),
        out_shape=(
            jax.ShapeDtypeStruct((slots * heads, head), bf16),
            jax.ShapeDtypeStruct((n // roles * slots, columns), bf16),
        ),
        in_specs=[anywhere, vmem, anywhere, vmem, vmem, anywhere, anywhere] + [vmem] + [smem] * 4,
        out_specs=(vmem, vmem),
        scratch_shapes=[
            pltpu.VMEM((rows, width), bf16),
            pltpu.VMEM((width * local_heads * 2, head), bf16),
            pltpu.VMEM((2, 128 * local_heads * 2, head), f32),
            pltpu.VMEM((width, local_heads * 2 * head), bf16),
            pltpu.VMEM((rows, head), f32),
            pltpu.VMEM((rows, head), f32),
            pltpu.VMEM((slots * line, head), bf16),
            pltpu.VMEM((heads * head, columns), bf16),
            pltpu.VMEM((roles - 1, heads * head, columns), bf16),
            pltpu.VMEM((rows, width), bf16),
            pltpu.VMEM((rows, local_heads * 2 * head), f32),
            pltpu.VMEM((local_heads, rows, head), bf16),
            pltpu.VMEM((local_heads, rows, head), bf16),
            pltpu.VMEM((n, slots * heads, head), bf16),
            pltpu.VMEM((n, padded, head), bf16),
            pltpu.VMEM((n, 8, padded), f32),
            pltpu.VMEM((used, head), bf16),
            pltpu.VMEM((8, padded), f32),
            pltpu.VMEM((slots * heads, line), f32),
            pltpu.VMEM((slots * heads, head), f32),
            pltpu.VMEM((slots * heads, head), f32),
            pltpu.VMEM((slots, heads * head), bf16),
            pltpu.VMEM((roles, n // roles, slots, heads * head), bf16),
            dma((CHUNKS + 2,)),
            dma((CHUNKS,)),
            dma((n // inner, inner)),
            dma((n,)),
            dma((n // inner, inner)),
            dma((n,)),
            dma((n // inner, inner)),
            dma((n,)),
            dma((n // inner, inner)),
            dma((roles, n // inner // roles, inner)),
            dma((roles, n // roles)),
            dma((roles - 1,)),
            dma((roles - 1,)),
        ],
        compiler_params=pltpu.CompilerParams(
            collective_id=0, has_side_effects=True, vmem_limit_bytes=56 * 1024 * 1024
        ),
    )(
        prompt_hidden,
        norm_gain.reshape(1, width),
        kv_weight.reshape(width * local_heads * 2, head),
        queries.reshape(slots * heads, head),
        new_kv.reshape(slots * local_heads * 2, head),
        response_cache.reshape(slots * line, head),
        out_weight.reshape(heads * head, columns),
        freq,
        prompt_excess,
        prompt_owner,
        response_counts,
        positions,
    )
    return (attended.reshape(slots, heads, head), block_out)


def solution(mesh):
    return jax.shard_map(
        on_device,
        mesh=mesh,
        in_specs=(
            P(("groups", "dev"), None),
            P(),
            P(None, "role", None, None),
            P("groups"),
            P("groups"),
            P("groups"),
            P(("groups", "dev"), "role", None),
            P(("groups", "dev"), "role", None, None),
            P(("groups", "dev"), None, "role", None, None),
            P(("groups", "dev")),
            P("role", None, "dev"),
        ),
        out_specs=(P(("groups", "dev"), "role", None), P(("groups", "role"), "dev")),
        check_vma=False,
    )
```

```python
import functools

import jax
import jax.numpy as jnp
import numpy as np
from jax import lax
from jax.experimental import pallas as pl
from jax.experimental.pallas import tpu as pltpu
from jax.sharding import PartitionSpec as P

RESP = 5
PROMPT_MIN = 512
MESH = pl.DeviceIdType.MESH
LOW = -1e30
CHUNKS = 4

rope_base = 500000.0


def nt(a, b):
    return lax.dot_general(a, b, (((1,), (1,)), ((), ())), preferred_element_type=jnp.float32)


def nn(a, b):
    return jnp.dot(a, b, preferred_element_type=jnp.float32)


def kernel(
    cfg,
    hidden_hbm, gain_ref, kvw_hbm, q_ref, new_ref, cache_hbm, ow_hbm,
    freq_ref, excess_ref, owner_ref, count_ref, pos_ref,
    attended_ref, block_ref,
    hidden, kvx, wide, kvw, cos_ref, sin_ref, cache, ow, ow_far, normed, acc, keys, values, q_all,
    mix_all, stat_all, mix_mine, stat_mine, scores, cache_mix, att_rows, att_flat, att_all,
    local_sem, cache_sem, q_send, q_recv, mix_send, mix_recv, stat_send, stat_recv,
    att_send, att_pass, att_recv, ow_send, ow_recv,
):
    n, inner, roles, slots, heads, local_heads, context, head, reach, used, padded = cfg
    outer = n // inner
    group = heads // local_heads
    per = n // roles
    rows = slots * heads
    scale = head ** (-0.5)
    me = lax.axis_index("dev")
    role = lax.axis_index("role")
    width = hidden.shape[1]
    step = width // CHUNKS
    pairs = 2 * local_heads
    tokens = hidden.shape[0]
    prompts = excess_ref.shape[0]
    i32 = jnp.int32
    major, minor = me // inner, lax.rem(me, inner)
    span = cache.shape[0] // CHUNKS

    hidden_copy = pltpu.make_async_copy(hidden_hbm, hidden, local_sem.at[CHUNKS])
    hidden_copy.start()
    kvw_copies = []
    for c in range(CHUNKS):
        part = pl.ds(c * step * pairs, step * pairs)
        kvw_copies.append(pltpu.make_async_copy(kvw_hbm.at[part], kvx.at[part], local_sem.at[c]))
        kvw_copies[-1].start()
    ow_copy = pltpu.make_async_copy(ow_hbm, ow, local_sem.at[CHUNKS + 1])
    ow_copy.start()
    cache_copies = []
    for c in range(CHUNKS):
        part = pl.ds(c * span, span)
        cache_copies.append(
            pltpu.make_async_copy(cache_hbm.at[part], cache.at[part], cache_sem.at[c])
        )
        cache_copies[-1].start()

    barrier = pltpu.get_barrier_semaphore()

    def greet(i, carry):
        other = lax.rem(me * roles + role + i, n * roles)
        pl.semaphore_signal(
            barrier,
            inc=1,
            device_id={"dev": other // roles, "role": lax.rem(other, roles)},
            device_id_type=MESH,
        )
        return carry

    lax.fori_loop(1, n * roles, greet, 0)

    lengths = [PROMPT_MIN + excess_ref[p] for p in range(prompts)]
    ends = [lengths[0]]
    for p in range(1, prompts):
        ends.append(ends[-1] + lengths[p])
    owners = [owner_ref[p] for p in range(prompts)]
    counts = [count_ref[p] for p in range(prompts)]
    firsts = []
    for p in range(prompts):
        first = jnp.int32(0)
        for q in range(p):
            first = first + jnp.where(owners[q] == owners[p], counts[q], 0)
        firsts.append(first)

    def prompt_of(token):
        found = jnp.zeros_like(token)
        for p in range(prompts):
            found = found + jnp.where(token >= ends[p], 1, 0)
        return found

    def reply_of(index):
        k = jnp.zeros_like(index)
        for m in range(1, local_heads):
            k = k + jnp.where(index >= m * (used // local_heads), 1, 0)
        rest = index - k * (used // local_heads)
        w = jnp.zeros_like(index)
        for m in range(1, reach):
            w = w + jnp.where(rest >= m * RESP * group, 1, 0)
        rest = rest - w * (RESP * group)
        return w, lax.div(rest, group), k * group + lax.rem(rest, group)

    first_prompt = prompt_of(me * tokens)
    w_of, r_of, h_of = reply_of(lax.broadcasted_iota(i32, (used, 128), 0))
    seat = jnp.zeros_like(w_of)
    number = jnp.zeros_like(w_of)
    for p in range(prompts):
        here = first_prompt + w_of == p
        seat = jnp.where(here, owners[p] * slots + firsts[p], seat)
        number = jnp.where(here, counts[p], number)
    live = r_of < number
    target = jnp.where(live, (seat + r_of) * heads + h_of, -1)
    seen = jnp.where(live, w_of, -1)
    window = prompt_of(me * tokens + lax.broadcasted_iota(i32, (8, tokens), 1)) - first_prompt
    col_first = prompt_of(tokens * lax.broadcasted_iota(i32, (n, padded), 0))
    col_index = lax.broadcasted_iota(i32, (n, padded), 1)
    cw, cr, ch = reply_of(col_index)
    col_code = jnp.where(col_index < used, ((col_first + cw) * RESP + cr) * heads + ch, -2)
    row_index = lax.broadcasted_iota(i32, (rows, 128), 0)
    row_slot = lax.div(row_index, heads)
    row_code = jnp.full((rows, 128), -1, i32)
    for p in range(prompts):
        rank = row_slot - firsts[p]
        mine = (owners[p] == me) & (rank >= 0) & (rank < counts[p])
        row_code = jnp.where(mine, (p * RESP + rank) * heads + lax.rem(row_index, heads), row_code)

    half = head // 2
    token = me * tokens + lax.broadcasted_iota(i32, (tokens, head), 0)
    offset = token
    for p in range(prompts):
        offset = offset - jnp.where(token >= ends[p], lengths[p], 0)
    angle = offset.astype(jnp.float32) * freq_ref[...]
    cos_ref[...] = jnp.cos(angle)
    lane = lax.broadcasted_iota(i32, (tokens, head), 1)
    sine = jnp.sin(angle)
    sin_ref[...] = jnp.where(lane < half, -sine, sine)
    for e in range(n):
        mix_all[e, used:padded, :] = jnp.zeros((padded - used, head), jnp.bfloat16)

    pl.semaphore_wait(barrier, n * roles - 1)

    def peer_at(o, i):
        return lax.rem(major + o, outer) * inner + lax.rem(minor + i, inner)

    class Gather:
        def __init__(self, mine, everyone, send, recv):
            self.refs = mine, everyone, send, recv

        def copy(self, src, slot, o, i, peer):
            mine, everyone, send, recv = self.refs
            return pltpu.make_async_remote_copy(
                src_ref=src, dst_ref=everyone(slot), send_sem=send.at[o, i],
                recv_sem=recv.at[slot], device_id={"dev": peer}, device_id_type=MESH,
            )

        def own(self, o, i):
            return self.copy(self.refs[0], me, o, i, peer_at(o, i))

        def passed(self, o, i):
            slot = peer_at(o, 0)
            return self.copy(self.refs[1](slot), slot, o, i, peer_at(0, i))

        def start(self):
            for o in range(1, outer):
                self.own(o, 0).start()
            for i in range(1, inner):
                self.own(0, i).start()

        def forward(self):
            for o in range(1, outer):
                self.passed(o, 0).wait_recv()
                for i in range(1, inner):
                    self.passed(o, i).start()

        def finish(self):
            for o in range(outer):
                for i in range(1, inner):
                    slot = peer_at(o, i)
                    self.copy(self.refs[0], slot, 0, 0, me).wait_recv()

        def sent(self):
            for o in range(1, outer):
                self.own(o, 0).wait_send()
                for i in range(1, inner):
                    self.passed(o, i).wait_send()
            for i in range(1, inner):
                self.own(0, i).wait_send()

    q_net = Gather(q_ref, lambda e: q_all.at[e], q_send, q_recv)
    mix_net = Gather(mix_mine, lambda e: mix_all.at[e, pl.ds(0, used)], mix_send, mix_recv)
    stat_net = Gather(stat_mine, lambda e: stat_all.at[e], stat_send, stat_recv)
    q_net.start()
    q_all[me] = q_ref[...]

    def ow_far_copy(j):
        return pltpu.make_async_remote_copy(
            src_ref=ow_hbm, dst_ref=ow_far.at[j - 1], send_sem=ow_send.at[j - 1],
            recv_sem=ow_recv.at[j - 1],
            device_id={"role": lax.rem(role + roles - j, roles)}, device_id_type=MESH,
        )

    for j in range(1, roles):
        ow_far_copy(j).start()

    hidden_copy.wait()
    block = 32

    def normalise(i, carry):
        part = pl.ds(pl.multiple_of(i * block, block), block)
        x = hidden[part, :].astype(jnp.float32)
        ratio = lax.rsqrt(jnp.mean(x * x, axis=-1, keepdims=True) + 1e-05)
        normed[part, :] = (x * ratio * gain_ref[...]).astype(jnp.bfloat16)
        return carry

    lax.fori_loop(0, hidden.shape[0] // block, normalise, 0, unroll=2)
    q_net.forward()
    tall = wide.shape[1]

    def unweave(i, carry):
        short = tall // pairs
        for lot in range(2):
            at = 2 * i + lot
            wide[lot] = kvx[pl.ds(pl.multiple_of(at * tall, tall), tall), :].astype(jnp.float32)
        for lot in range(2):
            part = pl.ds(pl.multiple_of((2 * i + lot) * short, short), short)
            for m in range(pairs):
                kvw[part, m * head : (m + 1) * head] = wide[
                    lot, pl.ds(m, short, stride=pairs), :
                ].astype(jnp.bfloat16)
        return carry

    per_chunk = step * pairs // (2 * tall)
    for c in range(CHUNKS):
        kvw_copies[c].wait()
        lax.fori_loop(c * per_chunk, (c + 1) * per_chunk, unweave, 0)
        part = slice(c * step, (c + 1) * step)
        product = nn(normed[:, part], kvw[part, :])
        if c == 0:
            acc[...] = product
        else:
            acc[...] += product
    for k in range(local_heads):
        raw = acc[:, 2 * k * head : (2 * k + 1) * head]
        turned = jnp.concatenate([raw[:, head // 2 :], raw[:, : head // 2]], axis=1)
        keys[k] = (raw * cos_ref[...] + turned * sin_ref[...]).astype(jnp.bfloat16)
        values[k] = acc[:, (2 * k + 1) * head : (2 * k + 2) * head].astype(jnp.bfloat16)

    q_net.finish()
    column = lax.broadcasted_iota(jnp.int32, (used, rows), 1)
    chosen = jnp.concatenate(
        [(target[:, :1] - e * rows == column).astype(jnp.float32) for e in range(n)], axis=1
    ).astype(jnp.bfloat16)
    table = nn(chosen, q_all[...].reshape(n * rows, head)).astype(jnp.bfloat16)
    share = used // local_heads
    peaks, totals, mixes = [], [], []
    for k in range(local_heads):
        mine = slice(k * share, (k + 1) * share)
        valid = seen[mine, :1] == window[0:1, :]
        s = jnp.where(valid, nt(table[mine], keys[k]) * scale, LOW)
        peak = jnp.max(s, axis=1, keepdims=True)
        w = jnp.where(valid, jnp.exp(s - peak), 0.0)
        peaks.append(peak)
        totals.append(jnp.sum(w, axis=1, keepdims=True))
        mixes.append(nn(w.astype(jnp.bfloat16), values[k]))
    mix_mine[...] = jnp.concatenate(mixes, axis=0).astype(jnp.bfloat16)
    lane = lax.broadcasted_iota(jnp.int32, (used, padded), 1)
    stats = jnp.where(
        lane == 0, jnp.concatenate(peaks, axis=0), jnp.where(lane == 1, jnp.concatenate(totals, axis=0), 0.0)
    )
    stats = jnp.concatenate([stats, jnp.zeros((padded - used, padded), jnp.float32)], axis=0)
    stat_mine[...] = stats.T[:8]

    stat_net.start()
    mix_net.start()
    mix_all[me, 0:used, :] = mix_mine[...]
    stat_all[me] = stat_mine[...]

    for c in range(CHUNKS):
        cache_copies[c].wait()
    line = 2 * local_heads * context

    def score(s, carry):
        part = pl.ds(pl.multiple_of(s * heads, heads), heads)
        block_rows = pl.ds(pl.multiple_of(s * line, line), line)
        raw = nt(q_ref[part, :], cache[block_rows, :]) * scale
        held_here = lax.div(col, pairs) < pos_ref[s]
        scores[part, :] = jnp.where((lax.rem(col, pairs) == 2 * own_head) & held_here, raw, LOW)
        return carry

    col = lax.broadcasted_iota(i32, (heads, line), 1)
    own_head = lax.div(lax.broadcasted_iota(i32, (heads, line), 0), group)

    lax.fori_loop(0, slots, score, 0, unroll=4)
    stat_net.forward()
    mix_net.forward()
    s = scores[...]
    cache_peak = jnp.max(s, axis=1, keepdims=True)
    w = jnp.where(s > 0.5 * LOW, jnp.exp(s - cache_peak), 0.0)
    cache_total = jnp.sum(w, axis=1, keepdims=True)
    scores[...] = pltpu.roll(w, 1, 1)

    def mix(s, carry):
        part = pl.ds(pl.multiple_of(s * heads, heads), heads)
        block_rows = pl.ds(pl.multiple_of(s * line, line), line)
        cache_mix[part, :] = nn(scores[part, :].astype(jnp.bfloat16), cache[block_rows, :])
        return carry

    lax.fori_loop(0, slots, mix, 0, unroll=4)

    fresh = new_ref[...]
    near = nt(q_ref[...], fresh) * scale
    fcol = lax.broadcasted_iota(jnp.int32, near.shape, 1)
    frow = lax.broadcasted_iota(jnp.int32, near.shape, 0)
    pair = 2 * (frow // group)
    self_score = jnp.max(jnp.where(fcol == pair, near, LOW), axis=1, keepdims=True)

    stat_net.finish()
    mix_net.finish()
    row_code = row_code[:, :1]
    held = jnp.concatenate(
        [jnp.where(row_code == col_code[e : e + 1, :], stat_all[e, 0:1, :], LOW) for e in range(n)],
        axis=1,
    )
    totals_all = jnp.concatenate([stat_all[e, 1:2, :] for e in range(n)], axis=1)
    peak = jnp.maximum(jnp.maximum(cache_peak, self_score), jnp.max(held, axis=1, keepdims=True))
    weight = jnp.where(held > 0.5 * LOW, jnp.exp(held - peak), 0.0)
    total = jnp.sum(weight * totals_all, axis=1, keepdims=True)
    mixed = nn(weight.astype(jnp.bfloat16), mix_all[...].reshape(n * padded, head))
    cache_weight = jnp.exp(cache_peak - peak)
    self_weight = jnp.exp(self_score - peak)
    total = total + cache_total * cache_weight + self_weight
    mixed = mixed + cache_mix[...] * cache_weight
    mixed = mixed + nn(jnp.where(fcol == pair + 1, self_weight, 0.0).astype(jnp.bfloat16), fresh)
    att = mixed / total
    att_rows[...] = att
    attended_ref[...] = att.astype(jnp.bfloat16)
    for h in range(heads):
        att_flat[:, h * head : (h + 1) * head] = att_rows[pl.ds(h, slots, stride=heads), :].astype(
            jnp.bfloat16
        )

    home = me // per
    place = lax.rem(me, per)

    fold = outer // roles

    def att_copy(src, from_role, o, slot, sem, peer, peer_role):
        return pltpu.make_async_remote_copy(
            src_ref=src, dst_ref=att_all.at[from_role, slot], send_sem=sem,
            recv_sem=att_recv.at[from_role, slot],
            device_id={"dev": peer, "role": peer_role}, device_id_type=MESH,
        )

    def att_own(o, i):
        return att_copy(att_flat, role, o, place, att_send.at[o, i], peer_at(o, i), home)

    def att_passed(from_role, o, i):
        slot = o * inner + minor
        return att_copy(
            att_all.at[from_role, slot], from_role, o, slot,
            att_pass.at[from_role, o, i], peer_at(0, i), role,
        )

    for o in range(1, outer):
        att_own(o, 0).start()
    for i in range(1, inner):
        att_own(0, i).start()

    @pl.when(home != role)
    def _():
        att_own(0, 0).start()

    @pl.when(home == role)
    def _():
        att_all[role, place] = att_flat[...]

    for j in range(1, roles):
        ow_far_copy(j).wait()
    ow_copy.wait()

    for o in range(fold):
        for from_role in range(roles):

            @pl.when(role * fold + o != major)
            def _():
                att_passed(from_role, o, 0).wait_recv()
                for i in range(1, inner):
                    att_passed(from_role, o, i).start()

            @pl.when((role * fold + o == major) & (from_role != role))
            def _():
                att_passed(from_role, o, 0).wait_recv()

    for o in range(fold):
        for from_role in range(roles):
            for i in range(1, inner):
                slot = o * inner + lax.rem(minor + i, inner)
                att_copy(att_flat, from_role, o, slot, att_send.at[0, 0], me, role).wait_recv()

    out = nn(att_all[role].reshape(per * slots, heads * head), ow[...])
    for j in range(1, roles):
        far = lax.rem(role + j, roles)
        out = out + nn(att_all[far].reshape(per * slots, heads * head), ow_far[j - 1])
    block_ref[...] = out.astype(jnp.bfloat16)

    q_net.sent()
    stat_net.sent()
    mix_net.sent()
    for o in range(1, outer):
        att_own(o, 0).wait_send()
    for i in range(1, inner):
        att_own(0, i).wait_send()

    @pl.when(home != role)
    def _():
        att_own(0, 0).wait_send()

    for o in range(fold):

        @pl.when(role * fold + o != major)
        def _():
            for from_role in range(roles):
                for i in range(1, inner):
                    att_passed(from_role, o, i).wait_send()


def settle(attended_ref, block_ref, attended_out, block_out):
    attended_out[...] = attended_ref[...]
    block_out[...] = block_ref[...]


def on_device(
    prompt_hidden,
    norm_gain,
    kv_weight,
    prompt_excess,
    prompt_owner,
    response_counts,
    queries,
    new_kv,
    response_cache,
    positions,
    out_weight,
):
    n = lax.axis_size("dev")
    roles = lax.axis_size("role")
    rows, width = prompt_hidden.shape
    local_heads = kv_weight.shape[1]
    head = kv_weight.shape[3]
    slots, heads, _ = queries.shape
    group = heads // local_heads
    context = response_cache.shape[1]
    prompts = prompt_excess.shape[0]
    columns = out_weight.shape[2]
    reach = min(rows // PROMPT_MIN + 2, prompts)
    used = reach * RESP * heads
    padded = -(-used // 128) * 128
    inner = 1
    while inner * inner < n:
        inner *= 2
    half = head // 2
    freq = np.float32(rope_base) ** (-np.arange(half, dtype=np.float32) * np.float32(2.0 / head))
    freq = jnp.asarray(np.concatenate([freq, freq])[None, :].astype(np.float32))
    line = 2 * local_heads * context
    bf16, f32 = jnp.bfloat16, jnp.float32
    dma = pltpu.SemaphoreType.DMA
    anywhere = pl.BlockSpec(memory_space=pl.ANY)
    vmem = pl.BlockSpec(memory_space=pltpu.VMEM)
    smem = pl.BlockSpec(memory_space=pltpu.SMEM)
    cfg = (n, inner, roles, slots, heads, local_heads, context, head, reach, used, padded)
    attended, block_out = pl.pallas_call(
        functools.partial(kernel, cfg),
        out_shape=(
            jax.ShapeDtypeStruct((slots * heads, head), bf16),
            jax.ShapeDtypeStruct((n // roles * slots, columns), bf16),
        ),
        in_specs=[anywhere, vmem, anywhere, vmem, vmem, anywhere, anywhere] + [vmem] + [smem] * 4,
        out_specs=(vmem, vmem),
        scratch_shapes=[
            pltpu.VMEM((rows, width), bf16),
            pltpu.VMEM((width * local_heads * 2, head), bf16),
            pltpu.VMEM((2, 128 * local_heads * 2, head), f32),
            pltpu.VMEM((width, local_heads * 2 * head), bf16),
            pltpu.VMEM((rows, head), f32),
            pltpu.VMEM((rows, head), f32),
            pltpu.VMEM((slots * line, head), bf16),
            pltpu.VMEM((heads * head, columns), bf16),
            pltpu.VMEM((roles - 1, heads * head, columns), bf16),
            pltpu.VMEM((rows, width), bf16),
            pltpu.VMEM((rows, local_heads * 2 * head), f32),
            pltpu.VMEM((local_heads, rows, head), bf16),
            pltpu.VMEM((local_heads, rows, head), bf16),
            pltpu.VMEM((n, slots * heads, head), bf16),
            pltpu.VMEM((n, padded, head), bf16),
            pltpu.VMEM((n, 8, padded), f32),
            pltpu.VMEM((used, head), bf16),
            pltpu.VMEM((8, padded), f32),
            pltpu.VMEM((slots * heads, line), f32),
            pltpu.VMEM((slots * heads, head), f32),
            pltpu.VMEM((slots * heads, head), f32),
            pltpu.VMEM((slots, heads * head), bf16),
            pltpu.VMEM((roles, n // roles, slots, heads * head), bf16),
            dma((CHUNKS + 2,)),
            dma((CHUNKS,)),
            dma((n // inner, inner)),
            dma((n,)),
            dma((n // inner, inner)),
            dma((n,)),
            dma((n // inner, inner)),
            dma((n,)),
            dma((n // inner, inner)),
            dma((roles, n // inner // roles, inner)),
            dma((roles, n // roles)),
            dma((roles - 1,)),
            dma((roles - 1,)),
        ],
        compiler_params=pltpu.CompilerParams(
            collective_id=0, has_side_effects=True, vmem_limit_bytes=56 * 1024 * 1024
        ),
    )(
        prompt_hidden,
        norm_gain.reshape(1, width),
        kv_weight.reshape(width * local_heads * 2, head),
        queries.reshape(slots * heads, head),
        new_kv.reshape(slots * local_heads * 2, head),
        response_cache.reshape(slots * line, head),
        out_weight.reshape(heads * head, columns),
        freq,
        prompt_excess,
        prompt_owner,
        response_counts,
        positions,
    )
    attended, block_out = pl.pallas_call(
        settle,
        out_shape=(
            jax.ShapeDtypeStruct(attended.shape, bf16),
            jax.ShapeDtypeStruct(block_out.shape, bf16),
        ),
        in_specs=[vmem, vmem],
        out_specs=(vmem, vmem),
    )(attended, block_out)
    return (attended.reshape(slots, heads, head), block_out)


def solution(mesh):
    return jax.shard_map(
        on_device,
        mesh=mesh,
        in_specs=(
            P(("groups", "dev"), None),
            P(),
            P(None, "role", None, None),
            P("groups"),
            P("groups"),
            P("groups"),
            P(("groups", "dev"), "role", None),
            P(("groups", "dev"), "role", None, None),
            P(("groups", "dev"), None, "role", None, None),
            P(("groups", "dev")),
            P("role", None, "dev"),
        ),
        out_specs=(P(("groups", "dev"), "role", None), P(("groups", "role"), "dev")),
        check_vma=False,
    )
```
